256 devices in a mesh: row: 16 (over z, y_hi), col: 8 (over x, core), depth: 2 (over y_lo).
Axes of the slice: x: 4, y: 4 (y_hi: 2, y_lo: 2; y = y_hi * 2 + y_lo), z: 8, core: 2. Of those that a mesh axis runs over, the one named last changes fastest.
Arguments:
- heads_concat: bfloat16 [8192, 16384], P('row', ('depth', 'col')), may hold values from -6 to 6
- w_out: bfloat16 [16384, 7168], P(('depth', 'row'), 'col'), may hold values from -0.046875 to 0.046875
Outputs:
- projected: bfloat16 [8192, 7168], P('row', ('col', 'depth'))
The draws below stay inside these ranges and needn't reach their ends.
All inputs are finite; a program needn't handle non-finite values.
Results may differ from the reference program's by a relative error of at most 0.001.
Values may be sent and summed in bfloat16 or wider, within the bound.
A program may use at most 128 MiB of HBM per device.

```python
import jax
import jax.numpy as jnp

D = 7168
K = 16384
TOKENS = 8192


def block_levels(stream_key, dims, cuts, least, top_value):
    factor_of, own = 1.0, jax.random.fold_in(stream_key, 6)
    for dim, parts in cuts:
        draws = jnp.exp(jax.random.uniform(jax.random.fold_in(own, dim), (parts,), jnp.float32, least / len(cuts), top_value / len(cuts)))
        factor_of = factor_of * jnp.repeat(draws, dims[dim] // parts).reshape([-1 if axis == dim else 1 for axis in range(len(dims))])
    return factor_of


def bell_draw(stream_key, extent, scale, limit, pieces=(), held_as=jnp.bfloat16):
    values = scale * jax.random.normal(stream_key, extent, jnp.float32)
    if pieces:
        values = values * block_levels(stream_key, extent, pieces, -0.22, 0.18)
    return jnp.clip(values, -limit, limit).astype(held_as)


def setup_inputs(seed: int = 0) -> dict:
    key_of = jax.random.split(jax.random.key(seed), 3)
    return {
        "heads_concat": bell_draw(key_of[0], (TOKENS, K), 1.0, 6.0, ((0, 16), (1, 16))),
        "w_out": bell_draw(key_of[1], (K, D), K ** -0.5, 0.046875, ((0, 32), (1, 8))),
    }


def reference(heads_concat, w_out):
    product = jnp.dot(heads_concat, w_out, preferred_element_type=jnp.float32)
    return product.astype(jnp.bfloat16)
```

```python
import functools

import jax
import jax.numpy as jnp
from jax import lax
from jax.experimental import pallas as pl
from jax.experimental.pallas import tpu as pltpu
from jax.sharding import PartitionSpec as P

MESH = pl.DeviceIdType.MESH
F32 = jnp.float32
BF16 = jnp.bfloat16

Z_ORDER = (
    [(t, 0) for t in (0, 6, 1, 5)]
    + [(t, 1) for t in (0, 6, 1, 5)]
    + [(0, 2), (6, 2), (2, 0), (4, 0), (1, 2), (5, 2)]
    + [(0, 3), (6, 3), (2, 1), (4, 1), (1, 3), (5, 3), (3, 0)]
    + [(2, 2), (4, 2), (3, 1), (2, 3), (4, 3), (3, 2), (3, 3)]
)
TILE_US = 2.8
HALF_PIECE_US = 5.6
LATENCY_US = 2.2


class Plan:
    def __init__(self):
        self.steps = []

    def at(self, time, step):
        self.steps.append((time, len(self.steps), step))

    def run(self):
        for _, _, step in sorted(self.steps, key=lambda s: s[:2]):
            step()


def kernel(
    heads, w, out, a, b, c, x_out, x_fwd, packed, r_up, r_down, q_up, q_down,
    load_sem, zs, zr, xs, xr, ds, dr, es, er, ys, yr,
):
    row, col, depth = lax.axis_index("row"), lax.axis_index("col"), lax.axis_index("depth")
    z, hi, lo = row // 2, row % 2, depth
    y = hi * 2 + lo
    rows, kb = 512, 512
    half = rows // 2
    lower, upper = pl.ds(0, half), pl.ds(half, half)

    def z_peer(step):
        return (((z + 8 + step) % 8) * 2 + hi, col, depth)

    def x_peer(step):
        return (row, (col + 8 + 2 * step) % 8, depth)

    def y_at(step):
        return (y + 4 + step) % 4

    def y_peer(step):
        other = y_at(step)
        return (z * 2 + other // 2, col, other % 2)

    twin = (row, col + 1 - 2 * (col % 2), depth)
    twin_col = col + 1 - 2 * (col % 2)

    sent = []

    def send(src, dst, send_sem, recv_sem, to):
        copy = pltpu.make_async_remote_copy(
            src_ref=src, dst_ref=dst, send_sem=send_sem, recv_sem=recv_sem, device_id=to, device_id_type=MESH
        )
        copy.start()
        sent.append(copy)

    def arrived(dst, send_sem, recv_sem, frm):
        pltpu.make_async_remote_copy(
            src_ref=dst, dst_ref=dst, send_sem=send_sem, recv_sem=recv_sem, device_id=frm, device_id_type=MESH
        ).wait_recv()

    load_own = pltpu.make_async_copy(heads.at[:, pl.ds(pl.multiple_of(hi * kb, kb), kb)], a.at[col, hi], load_sem.at[0])
    load_other = pltpu.make_async_copy(heads.at[:, pl.ds(pl.multiple_of((1 - hi) * kb, kb), kb)], x_out, load_sem.at[1])
    load_w = [
        pltpu.make_async_copy(w.at[:, pl.ds(128 * t, 128)], b.at[t, z], load_sem.at[2 + t]) for t in range(7)
    ]
    own_order = [t for t, hop in Z_ORDER if hop == 0]
    load_w[own_order[0]].start()
    load_own.start()
    load_other.start()
    for t in own_order[1:]:
        load_w[t].start()

    barrier = pltpu.get_barrier_semaphore()
    peers = [z_peer(1), z_peer(-1), x_peer(1), x_peer(-1), y_peer(1), y_peer(-1), twin]
    for peer in peers:
        pl.semaphore_signal(barrier, inc=1, device_id=peer, device_id_type=MESH)
    pl.semaphore_wait(barrier, len(peers))

    plan = Plan()

    def z_view(t, origin_steps, way, split):
        block = b.at[t, (z + 8 - way * origin_steps) % 8]
        return block.at[lower if way == 1 else upper] if split else block

    def z_send(t, hop):
        for i, way in enumerate((1, -1)):
            view = z_view(t, hop, way, hop == 3)
            send(view, view, zs.at[i, t, hop], zr.at[i, t, hop], z_peer(way))

    def z_arrived(t, hop):
        for i, way in enumerate((1, -1)):
            arrived(z_view(t, hop + 1, way, hop == 3), zs.at[i, t, hop], zr.at[i, t, hop], z_peer(-way))

    def z_step(t, hop):
        if hop == 0:
            load_w[t].wait()
        else:
            z_arrived(t, hop - 1)
        z_send(t, hop)

    link_free, key, z_time = 0.0, 0.0, {}
    for t, hop in Z_ORDER:
        ready = z_time[t, hop - 1] if hop else 0.0
        key = max(key, ready)
        plan.at(key, functools.partial(z_step, t, hop))
        link_free = max(link_free, ready) + TILE_US * (0.5 if hop == 3 else 1.0)
        z_time[t, hop] = link_free + LATENCY_US

    def x_half(way, second):
        return lower if (way == 1) != second else upper

    own, other = hi, 1 - hi
    h_of = (own, other)

    def x_own(k, second):
        for i, way in enumerate((1, -1)):
            view = a.at[col, h_of[k], x_half(way, second)]
            send(view, view, xs.at[i, k, int(second)], xr.at[i, k, int(second)], x_peer(way))

    def from_x(k, i, way, part):
        steps = 1 if part < 2 else 2
        block = a.at[(col + 8 - 2 * way * steps) % 8, h_of[k]]
        return block.at[x_half(way, part == 1)]

    def x_arrived(k, part):
        for i, way in enumerate((1, -1)):
            arrived(from_x(k, i, way, part), xs.at[i, k, part], xr.at[i, k, part], x_peer(-way))

    def x_forward(k):
        x_arrived(k, 0)
        for i, way in enumerate((1, -1)):
            view = from_x(k, i, way, 0)
            send(view, view, xs.at[i, k, 2], xr.at[i, k, 2], x_peer(way))

    def twin_piece(column, k, n):
        if n == 0:
            return a.at[column, h_of[k]]
        way = 1 if n % 2 else -1
        if n <= 2:
            return a.at[(column + 8 - 2 * way) % 8, h_of[k]]
        return a.at[(column + 4) % 8, h_of[k], x_half(way, False)]

    def twin_send(k, n):
        view = twin_piece(col, k, n)
        send(view, view, ds.at[k, n], dr.at[k, n], twin)

    def twin_arrived(k, n):
        arrived(twin_piece(twin_col, k, n), ds.at[k, n], dr.at[k, n], twin)

    def own_heads():
        load_own.wait()
        x_own(0, False)
        x_own(0, True)
        twin_send(0, 0)

    def exchange():
        load_other.wait()
        send(x_out.at[lower], x_fwd.at[0], es.at[0, 0], er.at[0, 0], y_peer(1))
        send(x_out.at[upper], x_fwd.at[1], es.at[1, 0], er.at[1, 0], y_peer(-1))

    def exchange_forward():
        for i, way in enumerate((1, -1)):
            arrived(x_fwd.at[i], es.at[i, 0], er.at[i, 0], y_peer(-way))
            from_hi = y_at(-way) // 2
            send(
                x_fwd.at[i], a.at[col, from_hi, lower if way == 1 else upper], es.at[i, 1], er.at[i, 1], y_peer(way)
            )

    def exchanged():
        for i, way in enumerate((1, -1)):
            arrived(a.at[col, other, lower if way == 1 else upper], es.at[i, 1], er.at[i, 1], y_peer(-way))
        x_own(1, False)
        x_own(1, True)
        twin_send(1, 0)

    plan.at(0.0, own_heads)
    plan.at(0.0, exchange)
    e1 = HALF_PIECE_US + LATENCY_US
    plan.at(e1, exchange_forward)
    e2 = e1 + HALF_PIECE_US + LATENCY_US
    plan.at(e2, exchanged)

    def x_second(k):
        x_arrived(k, 1)
        twin_send(k, 1)
        twin_send(k, 2)

    def x_third(k):
        x_arrived(k, 2)
        twin_send(k, 3)
        twin_send(k, 4)

    def x_done(k):
        for n in range(5):
            twin_arrived(k, n)

    for k in range(2):
        x0 = 3 * k * HALF_PIECE_US + LATENCY_US
        plan.at(x0 + HALF_PIECE_US, functools.partial(x_forward, k))
        plan.at(x0 + 2 * HALF_PIECE_US, functools.partial(x_second, k))
        plan.at(x0 + 3 * HALF_PIECE_US, functools.partial(x_third, k))
        plan.at(x0 + 3 * HALF_PIECE_US + 2.0, functools.partial(x_done, k))
    heads_time = 6 * HALF_PIECE_US + LATENCY_US + 2.0

    def multiply(tiles, blocks, first):
        @pl.loop(0, 4)
        def _(i):
            h, at = i // 2, pl.ds(pl.multiple_of((i % 2) * half, half), half)
            total = None
            for k in blocks:
                index = k if len(blocks) == 8 else (z + k) % 8
                right = [b[t, index] for t in tiles]
                right = right[0] if len(tiles) == 1 else jnp.concatenate(right, axis=1)
                term = jnp.dot(a[index, h, at, :], right, preferred_element_type=F32)
                total = term if total is None else total + term
            for n, t in enumerate(tiles):
                part = total[:, 128 * n : 128 * (n + 1)]
                c[t, h, at, :] = part if first else c[t, h, at, :] + part

    pairs = ((0, 6), (1, 5), (2, 4))
    hi_up, hi_down = y_at(1) // 2, y_at(-1) // 2

    def pair_views(p):
        if p < 3:
            first, last = pairs[p]
            mine, theirs = first + lo * (last - first), last - lo * (last - first)
            return (lambda h: c.at[mine, h]), (lambda h: c.at[theirs, h]), half
        return (lambda h: packed.at[lo, h]), (lambda h: packed.at[1 - lo, h]), half // 2

    def recv(buffer, p):
        return buffer.at[p] if p < 3 else buffer.at[3, pl.ds(0, buffer.shape[1] // 2)]

    def sum_start(p):
        mine, theirs, n = pair_views(p)
        low, high = pl.ds(0, n), pl.ds(n, n)
        send(mine(other).at[low], recv(q_down, p), ys.at[p, 0], yr.at[p, 0], y_peer(1))
        send(mine(other).at[high], recv(q_up, p), ys.at[p, 1], yr.at[p, 1], y_peer(-1))
        send(theirs(hi_up).at[high], recv(r_down, p).at[high], ys.at[p, 2], yr.at[p, 2], y_peer(1))
        send(theirs(hi_down).at[low], recv(r_up, p).at[low], ys.at[p, 3], yr.at[p, 3], y_peer(-1))

    def sum_pass(p):
        _, theirs, n = pair_views(p)
        low, high = pl.ds(0, n), pl.ds(n, n)
        arrived(recv(q_down, p), ys.at[p, 0], yr.at[p, 0], y_peer(-1))
        block = theirs(hi_up).at[low]
        block[...] = block[...] + recv(q_down, p)[...]
        send(block, recv(r_down, p).at[low], ys.at[p, 4], yr.at[p, 4], y_peer(1))
        arrived(recv(q_up, p), ys.at[p, 1], yr.at[p, 1], y_peer(1))
        block = theirs(hi_down).at[high]
        block[...] = block[...] + recv(q_up, p)[...]
        send(block, recv(r_up, p).at[high], ys.at[p, 5], yr.at[p, 5], y_peer(-1))

    def sum_end(p):
        mine, _, n = pair_views(p)
        low, high = pl.ds(0, n), pl.ds(n, n)
        arrived(recv(r_down, p).at[high], ys.at[p, 2], yr.at[p, 2], y_peer(-1))
        arrived(recv(r_up, p).at[low], ys.at[p, 3], yr.at[p, 3], y_peer(1))
        arrived(recv(r_down, p).at[low], ys.at[p, 4], yr.at[p, 4], y_peer(-1))
        arrived(recv(r_up, p).at[high], ys.at[p, 5], yr.at[p, 5], y_peer(1))
        total = mine(hi)[...] + recv(r_down, p)[...] + recv(r_up, p)[...]
        total = total.astype(BF16)
        if p < 3:
            @pl.when(lo == 0)
            def _():
                out[:, 128 * p : 128 * (p + 1)] = total

            @pl.when(lo == 1)
            def _():
                start = 64 + 128 * (2 - p)
                out[:, start : start + 128] = total
        else:
            for side, start in ((0, 384), (1, 0)):
                @pl.when(lo == side)
                def _():
                    out[0:256, start : start + 64] = total[:, :64]
                    out[256:512, start : start + 64] = total[:, 64:]

    def pack():
        lane = lax.broadcasted_iota(jnp.int32, (half, 128), 1)
        for h in range(2):
            top, bottom = c[3, h, 0:half, :], c[3, h, half:rows, :]
            packed[0, h] = jnp.where(lane < 64, top, pltpu.roll(bottom, 64, 1))
            packed[1, h] = jnp.where(lane < 64, pltpu.roll(top, 64, 1), bottom)

    busy = 0.0
    for p, tiles in enumerate(pairs):
        def start(p=p, tiles=tiles):
            for t in tiles:
                z_arrived(t, 3)
            multiply(tiles, range(8), True)
            sum_start(p)

        when = max(heads_time, max(z_time[t, 3] for t in tiles))
        plan.at(when, start)
        begin = max(busy, when + 3.0)
        plan.at(begin + 2.8 + LATENCY_US, functools.partial(sum_pass, p))
        plan.at(begin + 8.4 + LATENCY_US, functools.partial(sum_end, p))
        busy = begin + 8.4

    def early():
        multiply((3,), (0, 1, 2, 3, 5, 6, 7), True)

    def late():
        z_arrived(3, 3)
        multiply((3,), (4,), False)
        pack()
        sum_start(3)
        sum_pass(3)
        sum_end(3)

    plan.at(z_time[3, 2] + 0.1, early)
    plan.at(1e9, late)

    plan.run()
    for copy in sent:
        copy.wait_send()


def solution(mesh):
    def per_device(heads, w):
        rows, features = heads.shape
        depth, columns = w.shape
        dma = pltpu.SemaphoreType.DMA
        return pl.pallas_call(
            kernel,
            out_shape=jax.ShapeDtypeStruct((rows, columns // 2), BF16),
            in_specs=[pl.BlockSpec(memory_space=pl.ANY)] * 2,
            out_specs=pl.BlockSpec(memory_space=pltpu.VMEM),
            scratch_shapes=[
                pltpu.VMEM((8, 2, 512, 512), BF16),
                pltpu.VMEM((7, 8, 512, 128), BF16),
                pltpu.VMEM((7, 2, 512, 128), F32),
                pltpu.VMEM((512, 512), BF16),
                pltpu.VMEM((2, 256, 512), BF16),
                pltpu.VMEM((2, 2, 256, 128), F32),
                pltpu.VMEM((4, 512, 128), F32),
                pltpu.VMEM((4, 512, 128), F32),
                pltpu.VMEM((4, 256, 128), F32),
                pltpu.VMEM((4, 256, 128), F32),
                dma((9,)),
                dma((2, 7, 4)),
                dma((2, 7, 4)),
                dma((2, 2, 3)),
                dma((2, 2, 3)),
                dma((2, 5)),
                dma((2, 5)),
                dma((2, 2)),
                dma((2, 2)),
                dma((4, 6)),
                dma((4, 6)),
            ],
            compiler_params=pltpu.CompilerParams(
                collective_id=0, has_side_effects=True, vmem_limit_bytes=60 * 2**20
            ),
            name="projection",
        )(heads, w)

    return jax.shard_map(
        per_device,
        mesh=mesh,
        in_specs=(P("row", ("depth", "col")), P(("depth", "row"), "col")),
        out_specs=P("row", ("col", "depth")),
        check_vma=False,
    )
```

```python
import functools

import jax
import jax.numpy as jnp
from jax import lax
from jax.experimental import pallas as pl
from jax.experimental.pallas import tpu as pltpu
from jax.sharding import PartitionSpec as P

MESH = pl.DeviceIdType.MESH
F32 = jnp.float32
BF16 = jnp.bfloat16

TILES, LAST = 7, 6
Z_ORDER = (
    [(0, 0, 0), (1, 0, 0), (2, 0, 0), (3, 0, 0), (0, 1, 0), (1, 1, 0), (2, 1, 0), (3, 1, 0), (0, 2, 0), (1, 2, 0)]
    + [(4, 0, 0), (2, 2, 0), (0, 3, 0), (1, 3, 0), (3, 2, 0), (4, 1, 0), (5, 0, 0), (2, 3, 0), (3, 3, 0), (4, 2, 0)]
    + [(5, 1, 0), (6, 0, 0), (4, 3, 0), (6, 0, 1), (5, 2, 0), (6, 1, 0), (6, 1, 1), (5, 3, 0), (6, 2, 0), (6, 2, 1)]
    + [(6, 3, 0)]
)
TILE_US = 2.85
HALF_PIECE_US = 6.0
LATENCY_US = 3.0
PASS_LATE_US = 1.0
END_LATE_US = 30.0


class Plan:
    def __init__(self):
        self.steps = []

    def at(self, time, step):
        self.steps.append((time, len(self.steps), step))

    def run(self):
        for _, _, step in sorted(self.steps, key=lambda s: s[:2]):
            step()


def kernel(
    heads, w, out, a, b, w_own, x_out, x_fwd, sums, r_up, r_down, q_up, q_down,
    load_sem, zs, zr, xs, xr, ds, dr, es, er, ys, yr,
):
    row, col, depth = lax.axis_index("row"), lax.axis_index("col"), lax.axis_index("depth")
    z, hi, lo = row // 2, row % 2, depth
    y = hi * 2 + lo
    rows, kb = 512, 512
    half = rows // 2
    lower, upper = pl.ds(0, half), pl.ds(half, half)

    def z_peer(step):
        return (((z + 8 + step) % 8) * 2 + hi, col, depth)

    def x_peer(step):
        return (row, (col + 8 + 2 * step) % 8, depth)

    def y_at(step):
        return (y + 4 + step) % 4

    def y_peer(step):
        other = y_at(step)
        return (z * 2 + other // 2, col, other % 2)

    twin = (row, col + 1 - 2 * (col % 2), depth)
    twin_col = col + 1 - 2 * (col % 2)

    sent = []

    def send(src, dst, send_sem, recv_sem, to):
        copy = pltpu.make_async_remote_copy(
            src_ref=src, dst_ref=dst, send_sem=send_sem, recv_sem=recv_sem, device_id=to, device_id_type=MESH
        )
        copy.start()
        sent.append(copy)

    def arrived(dst, send_sem, recv_sem, frm):
        pltpu.make_async_remote_copy(
            src_ref=dst, dst_ref=dst, send_sem=send_sem, recv_sem=recv_sem, device_id=frm, device_id_type=MESH
        ).wait_recv()

    load_own = pltpu.make_async_copy(heads.at[:, pl.ds(pl.multiple_of(hi * kb, kb), kb)], a.at[col, hi], load_sem.at[0])
    load_other = pltpu.make_async_copy(heads.at[:, pl.ds(pl.multiple_of((1 - hi) * kb, kb), kb)], x_out, load_sem.at[1])
    load_w = [
        pltpu.make_async_copy(w.at[:, pl.ds(128 * t, 128)], w_own.at[t], load_sem.at[2 + t]) for t in range(TILES)
    ]
    for t in (0, 3, 4, 1, 5, 2, 6):
        load_w[t].start()
    load_own.start()
    load_other.start()

    barrier = pltpu.get_barrier_semaphore()
    peers = [z_peer(1), z_peer(-1), x_peer(1), x_peer(-1), y_peer(1), y_peer(-1), twin]
    for peer in peers:
        pl.semaphore_signal(barrier, inc=1, device_id=peer, device_id_type=MESH)

    loaded = set()
    lane = lax.broadcasted_iota(jnp.int32, (rows, 128), 1)
    for t in range(TILES):
        left, right = t // 2, (TILES + t) // 2
        for n in (left, right):
            if n not in loaded:
                load_w[n].wait()
                loaded.add(n)
        if t % 2 == 0:
            b[t, z] = jnp.where(lane < 64, w_own[left].astype(F32), w_own[right].astype(F32)).astype(BF16)
        else:
            both = jnp.where(lane < 64, w_own[right].astype(F32), w_own[left].astype(F32))
            b[t, z] = pltpu.roll(both, 64, 1).astype(BF16)

    pl.semaphore_wait(barrier, len(peers))

    plan = Plan()

    def z_view(t, origin_steps, way, part, split):
        block = b.at[t, (z + 8 - way * origin_steps) % 8]
        return block.at[lower if (way == 1) == (part == 0) else upper] if split else block

    def z_slot(t, part):
        return t + part * (TILES - t)

    def z_send(t, hop, part):
        slot = z_slot(t, part)
        for i, way in enumerate((1, -1)):
            view = z_view(t, hop, way, part, t == LAST or hop == 3)
            send(view, view, zs.at[i, slot, hop], zr.at[i, slot, hop], z_peer(way))

    def z_arrived(t, hop, part):
        slot = z_slot(t, part)
        for i, way in enumerate((1, -1)):
            view = z_view(t, hop + 1, way, part, t == LAST or hop == 3)
            arrived(view, zs.at[i, slot, hop], zr.at[i, slot, hop], z_peer(-way))

    def z_step(t, hop, part):
        if hop:
            z_arrived(t, hop - 1, part)
        z_send(t, hop, part)

    link_free, key, z_time = 0.0, 0.0, {}
    for t, hop, part in Z_ORDER:
        ready = z_time[t, hop - 1, part] if hop else 0.0
        key = max(key, ready)
        plan.at(key, functools.partial(z_step, t, hop, part))
        link_free = max(link_free, ready) + TILE_US * (0.5 if hop == 3 or t == LAST else 1.0)
        z_time[t, hop, part] = link_free + LATENCY_US

    def x_half(way, second):
        return lower if (way == 1) != second else upper

    own, other = hi, 1 - hi
    h_of = (own, other)

    def x_own(k, second):
        for i, way in enumerate((1, -1)):
            view = a.at[col, h_of[k], x_half(way, second)]
            send(view, view, xs.at[i, k, int(second)], xr.at[i, k, int(second)], x_peer(way))

    def from_x(k, i, way, part):
        steps = 1 if part < 2 else 2
        block = a.at[(col + 8 - 2 * way * steps) % 8, h_of[k]]
        return block.at[x_half(way, part == 1)]

    def x_arrived(k, part):
        for i, way in enumerate((1, -1)):
            arrived(from_x(k, i, way, part), xs.at[i, k, part], xr.at[i, k, part], x_peer(-way))

    def x_forward(k):
        x_arrived(k, 0)
        for i, way in enumerate((1, -1)):
            view = from_x(k, i, way, 0)
            send(view, view, xs.at[i, k, 2], xr.at[i, k, 2], x_peer(way))

    def twin_piece(column, k, n):
        if n == 0:
            return a.at[column, h_of[k]]
        way = 1 if n % 2 else -1
        if n <= 2:
            return a.at[(column + 8 - 2 * way) % 8, h_of[k]]
        return a.at[(column + 4) % 8, h_of[k], x_half(way, False)]

    def twin_send(k, n):
        view = twin_piece(col, k, n)
        send(view, view, ds.at[k, n], dr.at[k, n], twin)

    def twin_arrived(k, n):
        arrived(twin_piece(twin_col, k, n), ds.at[k, n], dr.at[k, n], twin)

    def own_heads():
        load_own.wait()
        x_own(0, False)
        x_own(0, True)
        twin_send(0, 0)

    def exchange():
        load_other.wait()
        send(x_out.at[lower], x_fwd.at[0], es.at[0, 0], er.at[0, 0], y_peer(1))
        send(x_out.at[upper], x_fwd.at[1], es.at[1, 0], er.at[1, 0], y_peer(-1))

    def exchange_forward():
        for i, way in enumerate((1, -1)):
            arrived(x_fwd.at[i], es.at[i, 0], er.at[i, 0], y_peer(-way))
            from_hi = y_at(-way) // 2
            send(
                x_fwd.at[i], a.at[col, from_hi, lower if way == 1 else upper], es.at[i, 1], er.at[i, 1], y_peer(way)
            )

    def exchanged():
        for i, way in enumerate((1, -1)):
            arrived(a.at[col, other, lower if way == 1 else upper], es.at[i, 1], er.at[i, 1], y_peer(-way))
        x_own(1, False)
        x_own(1, True)
        twin_send(1, 0)

    plan.at(0.0, own_heads)
    plan.at(0.0, exchange)
    e1 = HALF_PIECE_US + LATENCY_US
    plan.at(e1, exchange_forward)
    e2 = e1 + HALF_PIECE_US + LATENCY_US
    plan.at(e2, exchanged)

    def x_second(k):
        x_arrived(k, 1)
        twin_send(k, 1)
        twin_send(k, 2)

    def x_third(k):
        x_arrived(k, 2)
        twin_send(k, 3)
        twin_send(k, 4)

    def x_done(k):
        for n in range(5):
            twin_arrived(k, n)

    for k in range(2):
        x0 = 3 * k * HALF_PIECE_US + LATENCY_US
        plan.at(x0 + HALF_PIECE_US, functools.partial(x_forward, k))
        plan.at(x0 + 2 * HALF_PIECE_US, functools.partial(x_second, k))
        plan.at(x0 + 3 * HALF_PIECE_US, functools.partial(x_third, k))
        plan.at(x0 + 3 * HALF_PIECE_US + 2.0, functools.partial(x_done, k))
    heads_time = 6 * HALF_PIECE_US + LATENCY_US + 2.0

    def multiply(tiles, blocks, first, h=None):
        size = half // len(tiles)
        per_head = half // size

        @pl.loop(0, (1 if h is not None else 2) * per_head)
        def _(i):
            head = i // per_head if h is None else h
            start = pl.multiple_of((i % per_head) * size, size)
            top_at, bottom_at = pl.ds(start, size), pl.ds(start + half, size)
            total = None
            for k in blocks:
                index = k if len(blocks) == 8 else (z + 8 + k) % 8
                right = [b[t, index] for t in tiles]
                right = right[0] if len(tiles) == 1 else jnp.concatenate(right, axis=1)
                left = jnp.concatenate([a[index, head, top_at, :], a[index, head, bottom_at, :]], axis=0)
                term = jnp.dot(left, right, preferred_element_type=F32)
                total = term if total is None else total + term
            lanes = lax.broadcasted_iota(jnp.int32, (size, 128), 1)
            for n, t in enumerate(tiles):
                top, bottom = total[:size, 128 * n : 128 * (n + 1)], total[size:, 128 * n : 128 * (n + 1)]
                new = (
                    jnp.where(lanes < 64, top, pltpu.roll(bottom, 64, 1)),
                    jnp.where(lanes < 64, pltpu.roll(top, 64, 1), bottom),
                )
                for side in range(2):
                    sums[t, side, head, top_at] = new[side] if first else sums[t, side, head, top_at] + new[side]

    hi_up, hi_down = y_at(1) // 2, y_at(-1) // 2
    low, high = pl.ds(0, 128), pl.ds(128, 128)

    def cuts(t):
        count = 2 if t == LAST else 1
        return [(n, n * 128 // count, 128 // count) for n in range(count)]

    def sum_mine(t):
        for n, at, size in cuts(t):
            here = pl.ds(at, size)
            send(sums.at[t, lo, other, here], q_down.at[t, here], ys.at[t, n], yr.at[t, n], y_peer(1))
            send(
                sums.at[t, lo, other, pl.ds(128 + at, size)], q_up.at[t, here], ys.at[t, 2 + n], yr.at[t, 2 + n], y_peer(-1)
            )

    def sum_theirs(t):
        send(sums.at[t, 1 - lo, hi_up, high], r_down.at[t, high], ys.at[t, 4], yr.at[t, 4], y_peer(1))
        send(sums.at[t, 1 - lo, hi_down, low], r_up.at[t, low], ys.at[t, 5], yr.at[t, 5], y_peer(-1))

    def sum_pass(t):
        for n, at, size in cuts(t):
            here, there = pl.ds(at, size), pl.ds(128 + at, size)
            arrived(q_down.at[t, here], ys.at[t, n], yr.at[t, n], y_peer(-1))
            sums[t, 1 - lo, hi_up, here] = sums[t, 1 - lo, hi_up, here] + q_down[t, here]
            send(sums.at[t, 1 - lo, hi_up, here], r_down.at[t, here], ys.at[t, 6 + n], yr.at[t, 6 + n], y_peer(1))
            arrived(q_up.at[t, here], ys.at[t, 2 + n], yr.at[t, 2 + n], y_peer(1))
            sums[t, 1 - lo, hi_down, there] = sums[t, 1 - lo, hi_down, there] + q_up[t, here]
            send(sums.at[t, 1 - lo, hi_down, there], r_up.at[t, there], ys.at[t, 8 + n], yr.at[t, 8 + n], y_peer(-1))

    def sum_end(t):
        arrived(r_down.at[t, high], ys.at[t, 4], yr.at[t, 4], y_peer(-1))
        arrived(r_up.at[t, low], ys.at[t, 5], yr.at[t, 5], y_peer(1))
        for n, at, size in cuts(t):
            here, there = pl.ds(at, size), pl.ds(128 + at, size)
            arrived(r_down.at[t, here], ys.at[t, 6 + n], yr.at[t, 6 + n], y_peer(-1))
            arrived(r_up.at[t, there], ys.at[t, 8 + n], yr.at[t, 8 + n], y_peer(1))
        total = (sums[t, lo, hi] + r_down[t] + r_up[t]).T.astype(BF16)
        out[64 * t : 64 * (t + 1), 0:half] = total[:64]
        out[64 * t : 64 * (t + 1), half:rows] = total[64:]

    def tiles_whole(tiles):
        for t in tiles:
            z_arrived(t, 3, 0)
        multiply(tiles, range(8), True)
        for t in tiles:
            sum_mine(t)
            sum_theirs(t)

    def tile_early(t):
        multiply((t,), (0, 1, 2, 3, 5, 6, 7), True)

    def tile_late(t):
        z_arrived(t, 3, 0)
        multiply((t,), (4,), False, other)
        sum_mine(t)
        multiply((t,), (4,), False, own)
        sum_theirs(t)

    def last_early():
        multiply((LAST,), (0, 1, 2, 6, 7), True)

    def last_middle():
        z_arrived(LAST, 2, 1)
        multiply((LAST,), (3, 5), False)

    y_free = 0.0

    def plan_sums(t, begin):
        first = max(y_free, begin)
        plan.at(first + 1.4 + LATENCY_US + PASS_LATE_US, functools.partial(sum_pass, t))
        plan.at(first + 4.2 + LATENCY_US + END_LATE_US, functools.partial(sum_end, t))
        return first + 4.2

    for tiles in ((0, 1), (2, 3)):
        when = max(heads_time, max(z_time[t, 3, 0] for t in tiles))
        plan.at(when, functools.partial(tiles_whole, tiles))
        for t in tiles:
            y_free = plan_sums(t, when + 2.5)
    for t in (4, 5):
        plan.at(z_time[t, 2, 0] + 0.1, functools.partial(tile_early, t))
        plan.at(z_time[t, 3, 0], functools.partial(tile_late, t))
        y_free = plan_sums(t, z_time[t, 3, 0] + 0.6)
    plan.at(z_time[LAST, 1, 1] + 0.1, last_early)
    plan.at(z_time[LAST, 2, 1] + 0.1, last_middle)
    plan.at(z_time[LAST, 3, 0], functools.partial(tile_late, LAST))
    plan.at(1e9, functools.partial(sum_pass, LAST))
    plan.at(1e9, functools.partial(sum_end, LAST))

    plan.run()
    for copy in sent:
        copy.wait_send()


def solution(mesh):
    def per_device(heads, w):
        rows, features = heads.shape
        depth, columns = w.shape
        dma = pltpu.SemaphoreType.DMA
        return pl.pallas_call(
            kernel,
            out_shape=jax.ShapeDtypeStruct((columns // 2, rows), BF16),
            in_specs=[pl.BlockSpec(memory_space=pl.ANY)] * 2,
            out_specs=pl.BlockSpec(memory_space=pltpu.VMEM),
            scratch_shapes=[
                pltpu.VMEM((8, 2, 512, 512), BF16),
                pltpu.VMEM((7, 8, 512, 128), BF16),
                pltpu.VMEM((7, 512, 128), BF16),
                pltpu.VMEM((512, 512), BF16),
                pltpu.VMEM((2, 256, 512), BF16),
                pltpu.VMEM((7, 2, 2, 256, 128), F32),
                pltpu.VMEM((7, 256, 128), F32),
                pltpu.VMEM((7, 256, 128), F32),
                pltpu.VMEM((7, 128, 128), F32),
                pltpu.VMEM((7, 128, 128), F32),
                dma((9,)),
                dma((2, 8, 4)),
                dma((2, 8, 4)),
                dma((2, 2, 3)),
                dma((2, 2, 3)),
                dma((2, 5)),
                dma((2, 5)),
                dma((2, 2)),
                dma((2, 2)),
                dma((7, 10)),
                dma((7, 10)),
            ],
            compiler_params=pltpu.CompilerParams(
                collective_id=0, has_side_effects=True, vmem_limit_bytes=56_000_000
            ),
            name="projection",
        )(heads, w).T

    return jax.shard_map(
        per_device,
        mesh=mesh,
        in_specs=(P("row", ("depth", "col")), P(("depth", "row"), "col")),
        out_specs=P("row", ("col", "depth")),
        check_vma=False,
    )
```

```python
import functools

import jax
import jax.numpy as jnp
from jax import lax
from jax.experimental import pallas as pl
from jax.experimental.pallas import tpu as pltpu
from jax.sharding import PartitionSpec as P

MESH = pl.DeviceIdType.MESH
F32 = jnp.float32
BF16 = jnp.bfloat16

TILES, LAST, SPLIT = 7, 6, (6,)
Z_ORDER = (
    (0, 0, 0), (1, 0, 0), (2, 0, 0), (3, 0, 0), (0, 1, 0), (1, 1, 0), (2, 1, 0), (3, 1, 0), (0, 2, 0), (1, 2, 0),
    (4, 0, 0), (2, 2, 0), (0, 3, 0), (1, 3, 0), (3, 2, 0), (4, 1, 0), (5, 0, 0), (2, 3, 0), (3, 3, 0), (4, 2, 0),
    (5, 1, 0), (6, 0, 0), (4, 3, 0), (6, 0, 1), (5, 2, 0), (6, 1, 0), (6, 1, 1), (5, 3, 0), (6, 2, 0), (6, 2, 1),
    (6, 3, 0),
)
LOAD_ORDER = (0, 3, 4, 1, 5, 2, 6)
TILE_US = 2.85
HALF_PIECE_US = 6.0
LATENCY_US = 3.0
PASS_LATE_US = 1.0
END_LATE_US = 9.0


class Plan:
    def __init__(self):
        self.steps = []

    def at(self, time, step):
        self.steps.append((time, len(self.steps), step))

    def run(self):
        for _, _, step in sorted(self.steps, key=lambda s: s[:2]):
            step()


def kernel(
    heads, w, out, a, b, w_own, x_out, x_fwd, sums, r_up, r_down, q_up, q_down,
    load_sem, zs, zr, xs, xr, ds, dr, es, er, ys, yr,
):
    row, col, depth = lax.axis_index("row"), lax.axis_index("col"), lax.axis_index("depth")
    z, hi, lo = row // 2, row % 2, depth
    y = hi * 2 + lo
    rows, kb = 512, 512
    half = rows // 2
    lower, upper = pl.ds(0, half), pl.ds(half, half)

    def z_peer(step):
        return (((z + 8 + step) % 8) * 2 + hi, col, depth)

    def x_peer(step):
        return (row, (col + 8 + 2 * step) % 8, depth)

    def y_at(step):
        return (y + 4 + step) % 4

    def y_peer(step):
        other = y_at(step)
        return (z * 2 + other // 2, col, other % 2)

    twin = (row, col + 1 - 2 * (col % 2), depth)
    twin_col = col + 1 - 2 * (col % 2)

    sent = []

    def send(src, dst, send_sem, recv_sem, to):
        copy = pltpu.make_async_remote_copy(
            src_ref=src, dst_ref=dst, send_sem=send_sem, recv_sem=recv_sem, device_id=to, device_id_type=MESH
        )
        copy.start()
        sent.append(copy)

    def arrived(dst, send_sem, recv_sem, frm):
        pltpu.make_async_remote_copy(
            src_ref=dst, dst_ref=dst, send_sem=send_sem, recv_sem=recv_sem, device_id=frm, device_id_type=MESH
        ).wait_recv()

    load_own = pltpu.make_async_copy(heads.at[:, pl.ds(pl.multiple_of(hi * kb, kb), kb)], a.at[col, hi], load_sem.at[0])
    load_other = pltpu.make_async_copy(heads.at[:, pl.ds(pl.multiple_of((1 - hi) * kb, kb), kb)], x_out, load_sem.at[1])
    load_w = [
        pltpu.make_async_copy(w.at[:, pl.ds(128 * t, 128)], w_own.at[t], load_sem.at[2 + t]) for t in range(TILES)
    ]
    for t in LOAD_ORDER:
        load_w[t].start()
    load_own.start()
    load_other.start()

    barrier = pltpu.get_barrier_semaphore()
    peers = [z_peer(1), z_peer(-1), x_peer(1), x_peer(-1), y_peer(1), y_peer(-1), twin]
    for peer in peers:
        pl.semaphore_signal(barrier, inc=1, device_id=peer, device_id_type=MESH)

    loaded = set()
    lane = lax.broadcasted_iota(jnp.int32, (rows, 128), 1)

    packed_tiles = []

    def pack_tile(t):
        packed_tiles.append(t)
        left, right = t // 2, (TILES + t) // 2
        for n in (left, right):
            if n not in loaded:
                load_w[n].wait()
                loaded.add(n)
        if t % 2 == 0:
            b[t, z] = jnp.where(lane < 64, w_own[left].astype(F32), w_own[right].astype(F32)).astype(BF16)
        else:
            both = jnp.where(lane < 64, w_own[right].astype(F32), w_own[left].astype(F32))
            b[t, z] = pltpu.roll(both, 64, 1).astype(BF16)

    own_order = list(dict.fromkeys(t for t, hop, part in Z_ORDER if hop == 0))
    for t in own_order[:2]:
        pack_tile(t)
    pl.semaphore_wait(barrier, len(peers))

    plan = Plan()

    def z_view(t, origin_steps, way, part, split):
        block = b.at[t, (z + 8 - way * origin_steps) % 8]
        return block.at[lower if (way == 1) == (part == 0) else upper] if split else block

    def z_slot(t, part):
        return TILES + SPLIT.index(t) if part else t

    def z_send(t, hop, part):
        slot = z_slot(t, part)
        for i, way in enumerate((1, -1)):
            view = z_view(t, hop, way, part, t in SPLIT or hop == 3)
            send(view, view, zs.at[i, slot, hop], zr.at[i, slot, hop], z_peer(way))

    def z_arrived(t, hop, part):
        slot = z_slot(t, part)
        for i, way in enumerate((1, -1)):
            view = z_view(t, hop + 1, way, part, t in SPLIT or hop == 3)
            arrived(view, zs.at[i, slot, hop], zr.at[i, slot, hop], z_peer(-way))

    def z_step(t, hop, part):
        if hop:
            z_arrived(t, hop - 1, part)
        z_send(t, hop, part)
        if hop == 0 and len(packed_tiles) < TILES:
            pack_tile(own_order[len(packed_tiles)])

    link_free, key, z_time = 0.0, 0.0, {}
    for t, hop, part in Z_ORDER:
        ready = z_time[t, hop - 1, part] if hop else 0.0
        key = max(key, ready)
        plan.at(key, functools.partial(z_step, t, hop, part))
        link_free = max(link_free, ready) + TILE_US * (0.5 if hop == 3 or t in SPLIT else 1.0)
        z_time[t, hop, part] = link_free + LATENCY_US

    def x_half(way, second):
        return lower if (way == 1) != second else upper

    own, other = hi, 1 - hi
    h_of = (own, other)

    def x_own(k, second):
        for i, way in enumerate((1, -1)):
            view = a.at[col, h_of[k], x_half(way, second)]
            send(view, view, xs.at[i, k, int(second)], xr.at[i, k, int(second)], x_peer(way))

    def from_x(k, i, way, part):
        steps = 1 if part < 2 else 2
        block = a.at[(col + 8 - 2 * way * steps) % 8, h_of[k]]
        return block.at[x_half(way, part == 1)]

    def x_arrived(k, part):
        for i, way in enumerate((1, -1)):
            arrived(from_x(k, i, way, part), xs.at[i, k, part], xr.at[i, k, part], x_peer(-way))

    def x_forward(k):
        x_arrived(k, 0)
        for i, way in enumerate((1, -1)):
            view = from_x(k, i, way, 0)
            send(view, view, xs.at[i, k, 2], xr.at[i, k, 2], x_peer(way))

    def twin_piece(column, k, n):
        if n == 0:
            return a.at[column, h_of[k]]
        way = 1 if n % 2 else -1
        if n <= 2:
            return a.at[(column + 8 - 2 * way) % 8, h_of[k]]
        return a.at[(column + 4) % 8, h_of[k], x_half(way, False)]

    def twin_send(k, n):
        view = twin_piece(col, k, n)
        send(view, view, ds.at[k, n], dr.at[k, n], twin)

    def twin_arrived(k, n):
        arrived(twin_piece(twin_col, k, n), ds.at[k, n], dr.at[k, n], twin)

    def own_heads():
        load_own.wait()
        x_own(0, False)
        x_own(0, True)
        twin_send(0, 0)

    def exchange():
        load_other.wait()
        send(x_out.at[lower], x_fwd.at[0], es.at[0, 0], er.at[0, 0], y_peer(1))
        send(x_out.at[upper], x_fwd.at[1], es.at[1, 0], er.at[1, 0], y_peer(-1))

    def exchange_forward():
        for i, way in enumerate((1, -1)):
            arrived(x_fwd.at[i], es.at[i, 0], er.at[i, 0], y_peer(-way))
            from_hi = y_at(-way) // 2
            send(
                x_fwd.at[i], a.at[col, from_hi, lower if way == 1 else upper], es.at[i, 1], er.at[i, 1], y_peer(way)
            )

    def exchanged():
        for i, way in enumerate((1, -1)):
            arrived(a.at[col, other, lower if way == 1 else upper], es.at[i, 1], er.at[i, 1], y_peer(-way))
        x_own(1, False)
        x_own(1, True)
        twin_send(1, 0)

    plan.at(0.0, own_heads)
    plan.at(0.0, exchange)
    e1 = HALF_PIECE_US + LATENCY_US
    plan.at(e1, exchange_forward)
    e2 = e1 + HALF_PIECE_US + LATENCY_US
    plan.at(e2, exchanged)

    def x_second(k):
        x_arrived(k, 1)
        twin_send(k, 1)
        twin_send(k, 2)

    def x_third(k):
        x_arrived(k, 2)
        twin_send(k, 3)
        twin_send(k, 4)

    def x_done(k):
        for n in range(5):
            twin_arrived(k, n)

    for k in range(2):
        x0 = 3 * k * HALF_PIECE_US + LATENCY_US
        plan.at(x0 + HALF_PIECE_US, functools.partial(x_forward, k))
        plan.at(x0 + 2 * HALF_PIECE_US, functools.partial(x_second, k))
        plan.at(x0 + 3 * HALF_PIECE_US, functools.partial(x_third, k))
        plan.at(x0 + 3 * HALF_PIECE_US + 2.0, functools.partial(x_done, k))
    heads_time = 6 * HALF_PIECE_US + LATENCY_US + 2.0

    def multiply(tiles, blocks, first, h=None):
        size = half // len(tiles)
        per_head = half // size

        @pl.loop(0, (1 if h is not None else 2) * per_head)
        def _(i):
            head = i // per_head if h is None else h
            start = pl.multiple_of((i % per_head) * size, size)
            top_at, bottom_at = pl.ds(start, size), pl.ds(start + half, size)
            total = None
            for k in blocks:
                index = k if len(blocks) == 8 else (z + 8 + k) % 8
                right = [b[t, index] for t in tiles]
                right = right[0] if len(tiles) == 1 else jnp.concatenate(right, axis=1)
                left = jnp.concatenate([a[index, head, top_at, :], a[index, head, bottom_at, :]], axis=0)
                term = jnp.dot(left, right, preferred_element_type=F32)
                total = term if total is None else total + term
            lanes = lax.broadcasted_iota(jnp.int32, (size, 128), 1)
            for n, t in enumerate(tiles):
                top, bottom = total[:size, 128 * n : 128 * (n + 1)], total[size:, 128 * n : 128 * (n + 1)]
                new = (
                    jnp.where(lanes < 64, top, pltpu.roll(bottom, 64, 1)),
                    jnp.where(lanes < 64, pltpu.roll(top, 64, 1), bottom),
                )
                for side in range(2):
                    sums[t, side, head, top_at] = new[side] if first else sums[t, side, head, top_at] + new[side]

    hi_up, hi_down = y_at(1) // 2, y_at(-1) // 2
    low, high = pl.ds(0, 128), pl.ds(128, 128)

    def cuts(t):
        count = 2 if t == LAST else 1
        return [(n, n * 128 // count, 128 // count) for n in range(count)]

    def sum_mine(t):
        for n, at, size in cuts(t):
            here = pl.ds(at, size)
            send(sums.at[t, lo, other, here], q_down.at[t, here], ys.at[t, n], yr.at[t, n], y_peer(1))
            send(
                sums.at[t, lo, other, pl.ds(128 + at, size)], q_up.at[t, here], ys.at[t, 2 + n], yr.at[t, 2 + n], y_peer(-1)
            )

    def sum_theirs(t):
        send(sums.at[t, 1 - lo, hi_up, high], r_down.at[t, high], ys.at[t, 4], yr.at[t, 4], y_peer(1))
        send(sums.at[t, 1 - lo, hi_down, low], r_up.at[t, low], ys.at[t, 5], yr.at[t, 5], y_peer(-1))

    def sum_pass(t):
        for n, at, size in cuts(t):
            here, there = pl.ds(at, size), pl.ds(128 + at, size)
            arrived(q_down.at[t, here], ys.at[t, n], yr.at[t, n], y_peer(-1))
            sums[t, 1 - lo, hi_up, here] = sums[t, 1 - lo, hi_up, here] + q_down[t, here]
            send(sums.at[t, 1 - lo, hi_up, here], r_down.at[t, here], ys.at[t, 6 + n], yr.at[t, 6 + n], y_peer(1))
            arrived(q_up.at[t, here], ys.at[t, 2 + n], yr.at[t, 2 + n], y_peer(1))
            sums[t, 1 - lo, hi_down, there] = sums[t, 1 - lo, hi_down, there] + q_up[t, here]
            send(sums.at[t, 1 - lo, hi_down, there], r_up.at[t, there], ys.at[t, 8 + n], yr.at[t, 8 + n], y_peer(-1))

    def sum_end(t):
        arrived(r_down.at[t, high], ys.at[t, 4], yr.at[t, 4], y_peer(-1))
        arrived(r_up.at[t, low], ys.at[t, 5], yr.at[t, 5], y_peer(1))
        for n, at, size in cuts(t):
            here, there = pl.ds(at, size), pl.ds(128 + at, size)
            arrived(r_down.at[t, here], ys.at[t, 6 + n], yr.at[t, 6 + n], y_peer(-1))
            arrived(r_up.at[t, there], ys.at[t, 8 + n], yr.at[t, 8 + n], y_peer(1))
        total = (sums[t, lo, hi] + r_down[t] + r_up[t]).T.astype(BF16)
        out[64 * t : 64 * (t + 1), 0:half] = total[:64]
        out[64 * t : 64 * (t + 1), half:rows] = total[64:]

    def tiles_whole(tiles):
        for t in tiles:
            z_arrived(t, 3, 0)
        multiply(tiles, range(8), True)
        for t in tiles:
            sum_mine(t)
            sum_theirs(t)

    def tile_early(t):
        multiply((t,), (0, 1, 2, 6, 7), True)

    def tile_middle(t):
        if t in SPLIT:
            z_arrived(t, 2, 1)
        multiply((t,), (3, 5), False)

    def tile_late(t):
        z_arrived(t, 3, 0)
        multiply((t,), (4,), False, other)
        sum_mine(t)
        multiply((t,), (4,), False, own)
        sum_theirs(t)

    y_free = 0.0

    def plan_sums(t, begin):
        first = max(y_free, begin)
        plan.at(first + 1.4 + LATENCY_US + PASS_LATE_US, functools.partial(sum_pass, t))
        plan.at(first + 4.2 + LATENCY_US + END_LATE_US if t < 4 else 2e9, functools.partial(sum_end, t))
        return first + 4.2

    for tiles in ((0, 1), (2, 3)):
        when = max(heads_time, max(z_time[t, 3, 0] for t in tiles))
        plan.at(when, functools.partial(tiles_whole, tiles))
        for t in tiles:
            y_free = plan_sums(t, when + 2.5)
    for t in (4, 5, 6):
        last_part = int(t in SPLIT)
        key = max(z_time[t, 1, last_part], heads_time + 3.0) + 0.1
        plan.at(key, functools.partial(tile_early, t))
        key = max(key, z_time[t, 2, last_part]) + 0.1
        plan.at(key, functools.partial(tile_middle, t))
        key = max(key, z_time[t, 3, 0]) + 0.1
        plan.at(key, functools.partial(tile_late, t))
        if t != LAST:
            y_free = plan_sums(t, key + 0.6)
    plan.at(1e9, functools.partial(sum_pass, LAST))
    plan.at(3e9, functools.partial(sum_end, LAST))

    plan.run()
    for copy in sent:
        copy.wait_send()


def solution(mesh):
    def per_device(heads, w):
        rows, features = heads.shape
        depth, columns = w.shape
        dma = pltpu.SemaphoreType.DMA
        return pl.pallas_call(
            kernel,
            out_shape=jax.ShapeDtypeStruct((columns // 2, rows), BF16),
            in_specs=[pl.BlockSpec(memory_space=pl.ANY)] * 2,
            out_specs=pl.BlockSpec(memory_space=pltpu.VMEM),
            scratch_shapes=[
                pltpu.VMEM((8, 2, 512, 512), BF16),
                pltpu.VMEM((7, 8, 512, 128), BF16),
                pltpu.VMEM((7, 512, 128), BF16),
                pltpu.VMEM((512, 512), BF16),
                pltpu.VMEM((2, 256, 512), BF16),
                pltpu.VMEM((7, 2, 2, 256, 128), F32),
                pltpu.VMEM((7, 256, 128), F32),
                pltpu.VMEM((7, 256, 128), F32),
                pltpu.VMEM((7, 128, 128), F32),
                pltpu.VMEM((7, 128, 128), F32),
                dma((9,)),
                dma((2, 10, 4)),
                dma((2, 10, 4)),
                dma((2, 2, 3)),
                dma((2, 2, 3)),
                dma((2, 5)),
                dma((2, 5)),
                dma((2, 2)),
                dma((2, 2)),
                dma((7, 10)),
                dma((7, 10)),
            ],
            compiler_params=pltpu.CompilerParams(
                collective_id=0, has_side_effects=True, vmem_limit_bytes=56_000_000
            ),
            name="projection",
        )(heads, w).T

    return jax.shard_map(
        per_device,
        mesh=mesh,
        in_specs=(P("row", ("depth", "col")), P(("depth", "row"), "col")),
        out_specs=P("row", ("col", "depth")),
        check_vma=False,
    )
```

```python
import functools

import jax
import jax.numpy as jnp
from jax import lax
from jax.experimental import pallas as pl
from jax.experimental.pallas import tpu as pltpu
from jax.sharding import PartitionSpec as P

MESH = pl.DeviceIdType.MESH
F32 = jnp.float32
BF16 = jnp.bfloat16

TILES, LAST, SPLIT = 7, 6, (6,)
Z_ORDER = (
    (0, 0, 0), (1, 0, 0), (2, 0, 0), (3, 0, 0), (0, 1, 0), (1, 1, 0), (2, 1, 0), (3, 1, 0), (0, 2, 0), (1, 2, 0),
    (4, 0, 0), (2, 2, 0), (0, 3, 0), (1, 3, 0), (3, 2, 0), (4, 1, 0), (5, 0, 0), (2, 3, 0), (3, 3, 0), (4, 2, 0),
    (5, 1, 0), (6, 0, 0), (6, 0, 1), (6, 0, 2), (6, 0, 3), (4, 3, 0), (5, 2, 0), (6, 1, 0), (6, 1, 1), (6, 1, 2),
    (6, 1, 3), (6, 2, 0), (6, 2, 1), (5, 3, 0), (6, 2, 2), (6, 2, 3), (6, 3, 0), (6, 3, 1),
)
PARTS = 4
LOAD_ORDER = (0, 3, 4, 1, 5, 2, 6)
TILE_US = 2.85
HALF_PIECE_US = 6.0
LATENCY_US = 3.0
PASS_LATE_US = 1.0
END_LATE_US = 9.0


class Plan:
    def __init__(self):
        self.steps = []

    def at(self, time, step):
        self.steps.append((time, len(self.steps), step))

    def run(self):
        for _, _, step in sorted(self.steps, key=lambda s: s[:2]):
            step()


def kernel(
    heads, w, out, a, b, w_own, x_out, x_fwd, sums, r_up, r_down, q_up, q_down,
    load_sem, zs, zr, xs, xr, ds, dr, es, er, ys, yr,
):
    row, col, depth = lax.axis_index("row"), lax.axis_index("col"), lax.axis_index("depth")
    z, hi, lo = row // 2, row % 2, depth
    y = hi * 2 + lo
    rows, kb = 512, 512
    half = rows // 2
    lower, upper = pl.ds(0, half), pl.ds(half, half)

    def z_peer(step):
        return (((z + 8 + step) % 8) * 2 + hi, col, depth)

    def x_peer(step):
        return (row, (col + 8 + 2 * step) % 8, depth)

    def y_at(step):
        return (y + 4 + step) % 4

    def y_peer(step):
        other = y_at(step)
        return (z * 2 + other // 2, col, other % 2)

    twin = (row, col + 1 - 2 * (col % 2), depth)
    twin_col = col + 1 - 2 * (col % 2)

    sent = []

    def send(src, dst, send_sem, recv_sem, to):
        copy = pltpu.make_async_remote_copy(
            src_ref=src, dst_ref=dst, send_sem=send_sem, recv_sem=recv_sem, device_id=to, device_id_type=MESH
        )
        copy.start()
        sent.append(copy)

    def arrived(dst, send_sem, recv_sem, frm):
        pltpu.make_async_remote_copy(
            src_ref=dst, dst_ref=dst, send_sem=send_sem, recv_sem=recv_sem, device_id=frm, device_id_type=MESH
        ).wait_recv()

    load_own = pltpu.make_async_copy(heads.at[:, pl.ds(pl.multiple_of(hi * kb, kb), kb)], a.at[col, hi], load_sem.at[0])
    load_other = pltpu.make_async_copy(heads.at[:, pl.ds(pl.multiple_of((1 - hi) * kb, kb), kb)], x_out, load_sem.at[1])
    load_w = [
        pltpu.make_async_copy(w.at[:, pl.ds(128 * t, 128)], w_own.at[t], load_sem.at[2 + t]) for t in range(TILES)
    ]
    for t in LOAD_ORDER:
        load_w[t].start()
    load_own.start()
    load_other.start()

    barrier = pltpu.get_barrier_semaphore()
    peers = [z_peer(1), z_peer(-1), x_peer(1), x_peer(-1), y_peer(1), y_peer(-1), twin]
    for peer in peers:
        pl.semaphore_signal(barrier, inc=1, device_id=peer, device_id_type=MESH)

    loaded = set()
    lane = lax.broadcasted_iota(jnp.int32, (rows, 128), 1)

    packed_tiles = []

    def pack_tile(t):
        packed_tiles.append(t)
        left, right = t // 2, (TILES + t) // 2
        for n in (left, right):
            if n not in loaded:
                load_w[n].wait()
                loaded.add(n)
        if t % 2 == 0:
            b[t, z] = jnp.where(lane < 64, w_own[left].astype(F32), w_own[right].astype(F32)).astype(BF16)
        else:
            both = jnp.where(lane < 64, w_own[right].astype(F32), w_own[left].astype(F32))
            b[t, z] = pltpu.roll(both, 64, 1).astype(BF16)

    own_order = list(dict.fromkeys(t for t, hop, part in Z_ORDER if hop == 0))
    for t in own_order[:2]:
        pack_tile(t)
    pl.semaphore_wait(barrier, len(peers))

    plan = Plan()

    def z_view(t, origin_steps, way, part, hop):
        block = b.at[t, (z + 8 - way * origin_steps) % 8]
        if t in SPLIT:
            size = rows // PARTS
            at = part * size
            return block.at[pl.ds(at if way == 1 else (at + half) % rows, size)]
        return block.at[lower if way == 1 else upper] if hop == 3 else block

    def z_slot(t, part):
        return TILES - 1 + part if part else t

    def z_send(t, hop, part, i, way):
        slot = z_slot(t, part)
        view = z_view(t, hop, way, part, hop)
        send(view, view, zs.at[i, slot, hop], zr.at[i, slot, hop], z_peer(way))

    def z_arrived_one(t, hop, part, i, way):
        slot = z_slot(t, part)
        view = z_view(t, hop + 1, way, part, hop)
        arrived(view, zs.at[i, slot, hop], zr.at[i, slot, hop], z_peer(-way))

    def z_arrived(t, hop, parts):
        for part in parts:
            for i, way in enumerate((1, -1)):
                z_arrived_one(t, hop, part, i, way)

    def z_step(t, hop, part):
        for i, way in enumerate((1, -1)):
            if hop:
                z_arrived_one(t, hop - 1, part, i, way)
            z_send(t, hop, part, i, way)
        if hop == 0 and len(packed_tiles) < TILES:
            pack_tile(own_order[len(packed_tiles)])

    def parts_of(t, hop):
        return range(PARTS // (2 if hop == 3 else 1)) if t in SPLIT else (0,)

    link_free, key, z_time, z_key = 0.0, 0.0, {}, {}
    for t, hop, part in Z_ORDER:
        ready = z_time[t, hop - 1, part] if hop else 0.0
        key = max(key, ready)
        z_key[t, hop, part] = key
        plan.at(key, functools.partial(z_step, t, hop, part))
        link_free = max(link_free, ready) + TILE_US * (1.0 / PARTS if t in SPLIT else 0.5 if hop == 3 else 1.0)
        z_time[t, hop, part] = link_free + LATENCY_US

    def x_half(way, second):
        return lower if (way == 1) != second else upper

    own, other = hi, 1 - hi
    h_of = (own, other)

    def x_own(k, second):
        for i, way in enumerate((1, -1)):
            view = a.at[col, h_of[k], x_half(way, second)]
            send(view, view, xs.at[i, k, int(second)], xr.at[i, k, int(second)], x_peer(way))

    def from_x(k, i, way, part):
        steps = 1 if part < 2 else 2
        block = a.at[(col + 8 - 2 * way * steps) % 8, h_of[k]]
        return block.at[x_half(way, part == 1)]

    def x_arrived(k, part):
        for i, way in enumerate((1, -1)):
            arrived(from_x(k, i, way, part), xs.at[i, k, part], xr.at[i, k, part], x_peer(-way))

    def x_forward(k):
        x_arrived(k, 0)
        for i, way in enumerate((1, -1)):
            view = from_x(k, i, way, 0)
            send(view, view, xs.at[i, k, 2], xr.at[i, k, 2], x_peer(way))

    def twin_piece(column, k, n):
        if n == 0:
            return a.at[column, h_of[k]]
        way = 1 if n % 2 else -1
        if n <= 2:
            return a.at[(column + 8 - 2 * way) % 8, h_of[k]]
        return a.at[(column + 4) % 8, h_of[k], x_half(way, False)]

    def twin_send(k, n):
        view = twin_piece(col, k, n)
        send(view, view, ds.at[k, n], dr.at[k, n], twin)

    def twin_arrived(k, n):
        arrived(twin_piece(twin_col, k, n), ds.at[k, n], dr.at[k, n], twin)

    def own_heads():
        load_own.wait()
        x_own(0, False)
        x_own(0, True)
        twin_send(0, 0)

    def exchange():
        load_other.wait()
        send(x_out.at[lower], x_fwd.at[0], es.at[0, 0], er.at[0, 0], y_peer(1))
        send(x_out.at[upper], x_fwd.at[1], es.at[1, 0], er.at[1, 0], y_peer(-1))

    def exchange_forward():
        for i, way in enumerate((1, -1)):
            arrived(x_fwd.at[i], es.at[i, 0], er.at[i, 0], y_peer(-way))
            from_hi = y_at(-way) // 2
            send(
                x_fwd.at[i], a.at[col, from_hi, lower if way == 1 else upper], es.at[i, 1], er.at[i, 1], y_peer(way)
            )

    def exchanged():
        for i, way in enumerate((1, -1)):
            arrived(a.at[col, other, lower if way == 1 else upper], es.at[i, 1], er.at[i, 1], y_peer(-way))
        x_own(1, False)
        x_own(1, True)
        twin_send(1, 0)

    plan.at(0.0, own_heads)
    plan.at(0.0, exchange)
    e1 = HALF_PIECE_US + LATENCY_US
    plan.at(e1, exchange_forward)
    e2 = e1 + HALF_PIECE_US + LATENCY_US
    plan.at(e2, exchanged)

    def x_second(k):
        x_arrived(k, 1)
        twin_send(k, 1)
        twin_send(k, 2)

    def x_third(k):
        x_arrived(k, 2)
        twin_send(k, 3)
        twin_send(k, 4)

    def x_done(k):
        for n in range(5):
            twin_arrived(k, n)

    for k in range(2):
        x0 = 3 * k * HALF_PIECE_US + LATENCY_US
        plan.at(x0 + HALF_PIECE_US, functools.partial(x_forward, k))
        plan.at(x0 + 2 * HALF_PIECE_US, functools.partial(x_second, k))
        plan.at(x0 + 3 * HALF_PIECE_US, functools.partial(x_third, k))
        plan.at(x0 + 3 * HALF_PIECE_US + 2.0, functools.partial(x_done, k))
    heads_time = 6 * HALF_PIECE_US + LATENCY_US + 2.0

    def multiply(tiles, blocks, first, h=None):
        size = half // len(tiles)
        per_head = half // size

        @pl.loop(0, (1 if h is not None else 2) * per_head)
        def _(i):
            head = i // per_head if h is None else h
            start = pl.multiple_of((i % per_head) * size, size)
            top_at, bottom_at = pl.ds(start, size), pl.ds(start + half, size)
            total = None
            for k in blocks:
                index = k if len(blocks) == 8 else (z + 8 + k) % 8
                right = [b[t, index] for t in tiles]
                right = right[0] if len(tiles) == 1 else jnp.concatenate(right, axis=1)
                left = jnp.concatenate([a[index, head, top_at, :], a[index, head, bottom_at, :]], axis=0)
                term = jnp.dot(left, right, preferred_element_type=F32)
                total = term if total is None else total + term
            lanes = lax.broadcasted_iota(jnp.int32, (size, 128), 1)
            for n, t in enumerate(tiles):
                top, bottom = total[:size, 128 * n : 128 * (n + 1)], total[size:, 128 * n : 128 * (n + 1)]
                new = (
                    jnp.where(lanes < 64, top, pltpu.roll(bottom, 64, 1)),
                    jnp.where(lanes < 64, pltpu.roll(top, 64, 1), bottom),
                )
                for side in range(2):
                    sums[t, side, head, top_at] = new[side] if first else sums[t, side, head, top_at] + new[side]

    hi_up, hi_down = y_at(1) // 2, y_at(-1) // 2
    low, high = pl.ds(0, 128), pl.ds(128, 128)

    def cuts(t):
        count = 2 if t == LAST else 1
        return [(n, n * 128 // count, 128 // count) for n in range(count)]

    def sum_mine(t):
        for n, at, size in cuts(t):
            here = pl.ds(at, size)
            send(sums.at[t, lo, other, here], q_down.at[t, here], ys.at[t, n], yr.at[t, n], y_peer(1))
            send(
                sums.at[t, lo, other, pl.ds(128 + at, size)], q_up.at[t, here], ys.at[t, 2 + n], yr.at[t, 2 + n], y_peer(-1)
            )

    def sum_theirs(t):
        send(sums.at[t, 1 - lo, hi_up, high], r_down.at[t, high], ys.at[t, 4], yr.at[t, 4], y_peer(1))
        send(sums.at[t, 1 - lo, hi_down, low], r_up.at[t, low], ys.at[t, 5], yr.at[t, 5], y_peer(-1))

    def sum_pass(t):
        for n, at, size in cuts(t):
            here, there = pl.ds(at, size), pl.ds(128 + at, size)
            arrived(q_down.at[t, here], ys.at[t, n], yr.at[t, n], y_peer(-1))
            sums[t, 1 - lo, hi_up, here] = sums[t, 1 - lo, hi_up, here] + q_down[t, here]
            send(sums.at[t, 1 - lo, hi_up, here], r_down.at[t, here], ys.at[t, 6 + n], yr.at[t, 6 + n], y_peer(1))
            arrived(q_up.at[t, here], ys.at[t, 2 + n], yr.at[t, 2 + n], y_peer(1))
            sums[t, 1 - lo, hi_down, there] = sums[t, 1 - lo, hi_down, there] + q_up[t, here]
            send(sums.at[t, 1 - lo, hi_down, there], r_up.at[t, there], ys.at[t, 8 + n], yr.at[t, 8 + n], y_peer(-1))

    def sum_end(t):
        arrived(r_down.at[t, high], ys.at[t, 4], yr.at[t, 4], y_peer(-1))
        arrived(r_up.at[t, low], ys.at[t, 5], yr.at[t, 5], y_peer(1))
        for n, at, size in cuts(t):
            here, there = pl.ds(at, size), pl.ds(128 + at, size)
            arrived(r_down.at[t, here], ys.at[t, 6 + n], yr.at[t, 6 + n], y_peer(-1))
            arrived(r_up.at[t, there], ys.at[t, 8 + n], yr.at[t, 8 + n], y_peer(1))
        total = (sums[t, lo, hi] + r_down[t] + r_up[t]).T.astype(BF16)
        out[64 * t : 64 * (t + 1), 0:half] = total[:64]
        out[64 * t : 64 * (t + 1), half:rows] = total[64:]

    def tiles_whole(tiles):
        for t in tiles:
            z_arrived(t, 3, (0,))
        multiply(tiles, range(8), True)
        for t in tiles:
            sum_mine(t)
            sum_theirs(t)

    def tile_early(t):
        multiply((t,), (0, 1, 2, 6, 7), True)

    def tile_middle(t):
        if t in SPLIT:
            z_arrived(t, 2, range(PARTS // 2, PARTS))
        multiply((t,), (3, 5), False)

    def tile_late(t):
        z_arrived(t, 3, parts_of(t, 3))
        multiply((t,), (4,), False, other)
        sum_mine(t)
        multiply((t,), (4,), False, own)
        sum_theirs(t)

    y_free = 0.0

    def plan_sums(t, begin):
        first = max(y_free, begin)
        plan.at(first + 1.4 + LATENCY_US + PASS_LATE_US, functools.partial(sum_pass, t))
        plan.at(first + 4.2 + LATENCY_US + END_LATE_US if t < 4 else 2e9, functools.partial(sum_end, t))
        return first + 4.2

    for tiles in ((0, 1), (2, 3)):
        when = max(heads_time, max(z_time[t, 3, 0] for t in tiles))
        plan.at(when, functools.partial(tiles_whole, tiles))
        for t in tiles:
            y_free = plan_sums(t, when + 2.5)
    for t in (4, 5, 6):
        last_part = parts_of(t, 2)[-1]
        key = max(z_time[t, 1, last_part], z_key[t, 2, last_part], heads_time + 3.0) + 0.1
        plan.at(key, functools.partial(tile_early, t))
        key = max(key, z_time[t, 2, last_part], z_key[t, 3, parts_of(t, 3)[-1]]) + 0.1
        plan.at(key, functools.partial(tile_middle, t))
        key = max(key, z_time[t, 3, parts_of(t, 3)[-1]]) + 0.1
        plan.at(key, functools.partial(tile_late, t))
        if t != LAST:
            y_free = plan_sums(t, key + 0.6)
    plan.at(1e9, functools.partial(sum_pass, LAST))
    plan.at(3e9, functools.partial(sum_end, LAST))

    plan.run()
    for copy in sent:
        copy.wait_send()


def solution(mesh):
    def per_device(heads, w):
        rows, features = heads.shape
        depth, columns = w.shape
        dma = pltpu.SemaphoreType.DMA
        return pl.pallas_call(
            kernel,
            out_shape=jax.ShapeDtypeStruct((columns // 2, rows), BF16),
            in_specs=[pl.BlockSpec(memory_space=pl.ANY)] * 2,
            out_specs=pl.BlockSpec(memory_space=pltpu.VMEM),
            scratch_shapes=[
                pltpu.VMEM((8, 2, 512, 512), BF16),
                pltpu.VMEM((7, 8, 512, 128), BF16),
                pltpu.VMEM((7, 512, 128), BF16),
                pltpu.VMEM((512, 512), BF16),
                pltpu.VMEM((2, 256, 512), BF16),
                pltpu.VMEM((7, 2, 2, 256, 128), F32),
                pltpu.VMEM((7, 256, 128), F32),
                pltpu.VMEM((7, 256, 128), F32),
                pltpu.VMEM((7, 128, 128), F32),
                pltpu.VMEM((7, 128, 128), F32),
                dma((9,)),
                dma((2, 10, 4)),
                dma((2, 10, 4)),
                dma((2, 2, 3)),
                dma((2, 2, 3)),
                dma((2, 5)),
                dma((2, 5)),
                dma((2, 2)),
                dma((2, 2)),
                dma((7, 10)),
                dma((7, 10)),
            ],
            compiler_params=pltpu.CompilerParams(
                collective_id=0, has_side_effects=True, vmem_limit_bytes=56_000_000
            ),
            name="projection",
        )(heads, w).T

    return jax.shard_map(
        per_device,
        mesh=mesh,
        in_specs=(P("row", ("depth", "col")), P(("depth", "row"), "col")),
        out_specs=P("row", ("col", "depth")),
        check_vma=False,
    )
```

```python
import functools

import jax
import jax.numpy as jnp
from jax import lax
from jax.experimental import pallas as pl
from jax.experimental.pallas import tpu as pltpu
from jax.sharding import PartitionSpec as P

MESH = pl.DeviceIdType.MESH
F32 = jnp.float32
BF16 = jnp.bfloat16

TILES, LAST, SPLIT = 7, 6, (6,)
Z_ORDER = (
    (0, 0, 0), (1, 0, 0), (2, 0, 0), (3, 0, 0), (0, 1, 0), (1, 1, 0), (2, 1, 0), (3, 1, 0), (0, 2, 0), (1, 2, 0),
    (4, 0, 0), (2, 2, 0), (0, 3, 0), (1, 3, 0), (3, 2, 0), (4, 1, 0), (5, 0, 0), (2, 3, 0), (3, 3, 0), (4, 2, 0),
    (5, 1, 0), (6, 0, 0), (6, 0, 1), (4, 3, 0), (5, 2, 0), (6, 1, 0), (6, 1, 1), (6, 2, 0), (5, 3, 0), (6, 2, 1),
    (6, 3, 0),
)
PARTS = 2
LOAD_ORDER = (0, 3, 4, 1, 5, 2, 6)
TILE_US = 2.85
HALF_PIECE_US = 6.0
LATENCY_US = 3.0
PASS_LATE_US = 1.0
END_LATE_US = 9.0


class Plan:
    def __init__(self):
        self.steps = []

    def at(self, time, step):
        self.steps.append((time, len(self.steps), step))

    def run(self):
        for _, _, step in sorted(self.steps, key=lambda s: s[:2]):
            step()


def kernel(
    heads, w, out, a, b, w_own, x_out, x_fwd, sums, r_up, r_down, q_up, q_down,
    load_sem, zs, zr, xs, xr, ds, dr, es, er, ys, yr,
):
    row, col, depth = lax.axis_index("row"), lax.axis_index("col"), lax.axis_index("depth")
    z, hi, lo = row // 2, row % 2, depth
    y = hi * 2 + lo
    rows, kb = 512, 512
    half = rows // 2
    lower, upper = pl.ds(0, half), pl.ds(half, half)

    def z_peer(step):
        return (((z + 8 + step) % 8) * 2 + hi, col, depth)

    def x_peer(step):
        return (row, (col + 8 + 2 * step) % 8, depth)

    def y_at(step):
        return (y + 4 + step) % 4

    def y_peer(step):
        other = y_at(step)
        return (z * 2 + other // 2, col, other % 2)

    twin = (row, col + 1 - 2 * (col % 2), depth)
    twin_col = col + 1 - 2 * (col % 2)

    sent = []

    def send(src, dst, send_sem, recv_sem, to):
        copy = pltpu.make_async_remote_copy(
            src_ref=src, dst_ref=dst, send_sem=send_sem, recv_sem=recv_sem, device_id=to, device_id_type=MESH
        )
        copy.start()
        sent.append(copy)

    def arrived(dst, send_sem, recv_sem, frm):
        pltpu.make_async_remote_copy(
            src_ref=dst, dst_ref=dst, send_sem=send_sem, recv_sem=recv_sem, device_id=frm, device_id_type=MESH
        ).wait_recv()

    load_own = pltpu.make_async_copy(heads.at[:, pl.ds(pl.multiple_of(hi * kb, kb), kb)], a.at[col, hi], load_sem.at[0])
    load_other = pltpu.make_async_copy(heads.at[:, pl.ds(pl.multiple_of((1 - hi) * kb, kb), kb)], x_out, load_sem.at[1])
    load_w = [
        pltpu.make_async_copy(w.at[:, pl.ds(128 * t, 128)], w_own.at[t], load_sem.at[2 + t]) for t in range(TILES)
    ]
    for t in LOAD_ORDER:
        load_w[t].start()
    load_own.start()
    load_other.start()

    barrier = pltpu.get_barrier_semaphore()
    peers = [z_peer(1), z_peer(-1), x_peer(1), x_peer(-1), y_peer(1), y_peer(-1), twin]
    for peer in peers:
        pl.semaphore_signal(barrier, inc=1, device_id=peer, device_id_type=MESH)

    loaded = set()
    lane = lax.broadcasted_iota(jnp.int32, (rows, 128), 1)

    packed_tiles = []

    def pack_tile(t):
        packed_tiles.append(t)
        left, right = t // 2, (TILES + t) // 2
        for n in (left, right):
            if n not in loaded:
                load_w[n].wait()
                loaded.add(n)
        if t % 2 == 0:
            b[t, z] = jnp.where(lane < 64, w_own[left].astype(F32), w_own[right].astype(F32)).astype(BF16)
        else:
            both = jnp.where(lane < 64, w_own[right].astype(F32), w_own[left].astype(F32))
            b[t, z] = pltpu.roll(both, 64, 1).astype(BF16)

    own_order = list(dict.fromkeys(t for t, hop, part in Z_ORDER if hop == 0))
    for t in own_order[:2]:
        pack_tile(t)
    pl.semaphore_wait(barrier, len(peers))

    plan = Plan()

    def z_view(t, origin_steps, way, part, hop):
        block = b.at[t, (z + 8 - way * origin_steps) % 8]
        if t in SPLIT:
            size = rows // PARTS
            at = part * size
            return block.at[pl.ds(at if way == 1 else (at + half) % rows, size)]
        return block.at[lower if way == 1 else upper] if hop == 3 else block

    def z_slot(t, part):
        return TILES - 1 + part if part else t

    def z_send(t, hop, part, i, way):
        slot = z_slot(t, part)
        view = z_view(t, hop, way, part, hop)
        send(view, view, zs.at[i, slot, hop], zr.at[i, slot, hop], z_peer(way))

    def z_arrived_one(t, hop, part, i, way):
        slot = z_slot(t, part)
        view = z_view(t, hop + 1, way, part, hop)
        arrived(view, zs.at[i, slot, hop], zr.at[i, slot, hop], z_peer(-way))

    def z_arrived(t, hop, parts):
        for part in parts:
            for i, way in enumerate((1, -1)):
                z_arrived_one(t, hop, part, i, way)

    def z_step(t, hop, part):
        for i, way in enumerate((1, -1)):
            if hop:
                z_arrived_one(t, hop - 1, part, i, way)
            z_send(t, hop, part, i, way)
        if hop == 0 and len(packed_tiles) < TILES:
            pack_tile(own_order[len(packed_tiles)])

    def parts_of(t, hop):
        return range(PARTS // (2 if hop == 3 else 1)) if t in SPLIT else (0,)

    link_free, key, z_time, z_key = 0.0, 0.0, {}, {}
    for t, hop, part in Z_ORDER:
        ready = z_time[t, hop - 1, part] if hop else 0.0
        key = max(key, ready)
        z_key[t, hop, part] = key
        plan.at(key, functools.partial(z_step, t, hop, part))
        link_free = max(link_free, ready) + TILE_US * (1.0 / PARTS if t in SPLIT else 0.5 if hop == 3 else 1.0)
        z_time[t, hop, part] = link_free + LATENCY_US

    def x_half(way, second):
        return lower if (way == 1) != second else upper

    own, other = hi, 1 - hi
    h_of = (own, other)

    def x_own(k, second):
        for i, way in enumerate((1, -1)):
            view = a.at[col, h_of[k], x_half(way, second)]
            send(view, view, xs.at[i, k, int(second)], xr.at[i, k, int(second)], x_peer(way))

    def from_x(k, i, way, part):
        steps = 1 if part < 2 else 2
        block = a.at[(col + 8 - 2 * way * steps) % 8, h_of[k]]
        return block.at[x_half(way, part == 1)]

    def x_arrived(k, part):
        for i, way in enumerate((1, -1)):
            arrived(from_x(k, i, way, part), xs.at[i, k, part], xr.at[i, k, part], x_peer(-way))

    def x_forward(k):
        x_arrived(k, 0)
        for i, way in enumerate((1, -1)):
            view = from_x(k, i, way, 0)
            send(view, view, xs.at[i, k, 2], xr.at[i, k, 2], x_peer(way))

    def twin_piece(column, k, n):
        if n == 0:
            return a.at[column, h_of[k]]
        way = 1 if n % 2 else -1
        if n <= 2:
            return a.at[(column + 8 - 2 * way) % 8, h_of[k]]
        return a.at[(column + 4) % 8, h_of[k], x_half(way, False)]

    def twin_send(k, n):
        view = twin_piece(col, k, n)
        send(view, view, ds.at[k, n], dr.at[k, n], twin)

    def twin_arrived(k, n):
        arrived(twin_piece(twin_col, k, n), ds.at[k, n], dr.at[k, n], twin)

    def own_heads():
        load_own.wait()
        x_own(0, False)
        x_own(0, True)
        twin_send(0, 0)

    def exchange():
        load_other.wait()
        send(x_out.at[lower], x_fwd.at[0], es.at[0, 0], er.at[0, 0], y_peer(1))
        send(x_out.at[upper], x_fwd.at[1], es.at[1, 0], er.at[1, 0], y_peer(-1))

    def exchange_forward():
        for i, way in enumerate((1, -1)):
            arrived(x_fwd.at[i], es.at[i, 0], er.at[i, 0], y_peer(-way))
            from_hi = y_at(-way) // 2
            send(
                x_fwd.at[i], a.at[col, from_hi, lower if way == 1 else upper], es.at[i, 1], er.at[i, 1], y_peer(way)
            )

    def exchanged():
        for i, way in enumerate((1, -1)):
            arrived(a.at[col, other, lower if way == 1 else upper], es.at[i, 1], er.at[i, 1], y_peer(-way))
        x_own(1, False)
        x_own(1, True)
        twin_send(1, 0)

    plan.at(0.0, own_heads)
    plan.at(0.0, exchange)
    e1 = HALF_PIECE_US + LATENCY_US
    plan.at(e1, exchange_forward)
    e2 = e1 + HALF_PIECE_US + LATENCY_US
    plan.at(e2, exchanged)

    def x_second(k):
        x_arrived(k, 1)
        twin_send(k, 1)
        twin_send(k, 2)

    def x_third(k):
        x_arrived(k, 2)
        twin_send(k, 3)
        twin_send(k, 4)

    def x_done(k):
        for n in range(5):
            twin_arrived(k, n)

    for k in range(2):
        x0 = 3 * k * HALF_PIECE_US + LATENCY_US
        plan.at(x0 + HALF_PIECE_US, functools.partial(x_forward, k))
        plan.at(x0 + 2 * HALF_PIECE_US, functools.partial(x_second, k))
        plan.at(x0 + 3 * HALF_PIECE_US, functools.partial(x_third, k))
        plan.at(x0 + 3 * HALF_PIECE_US + 2.0, functools.partial(x_done, k))
    heads_time = 6 * HALF_PIECE_US + LATENCY_US + 2.0

    def multiply(tiles, blocks, first, h=None):
        size = half // len(tiles)
        per_head = half // size

        @pl.loop(0, (1 if h is not None else 2) * per_head)
        def _(i):
            head = i // per_head if h is None else h
            start = pl.multiple_of((i % per_head) * size, size)
            top_at, bottom_at = pl.ds(start, size), pl.ds(start + half, size)
            total = None
            for k in blocks:
                index = k if len(blocks) == 8 else (z + 8 + k) % 8
                right = [b[t, index] for t in tiles]
                right = right[0] if len(tiles) == 1 else jnp.concatenate(right, axis=1)
                left = jnp.concatenate([a[index, head, top_at, :], a[index, head, bottom_at, :]], axis=0)
                term = jnp.dot(left, right, preferred_element_type=F32)
                total = term if total is None else total + term
            lanes = lax.broadcasted_iota(jnp.int32, (size, 128), 1)
            for n, t in enumerate(tiles):
                top, bottom = total[:size, 128 * n : 128 * (n + 1)], total[size:, 128 * n : 128 * (n + 1)]
                new = (
                    jnp.where(lanes < 64, top, pltpu.roll(bottom, 64, 1)),
                    jnp.where(lanes < 64, pltpu.roll(top, 64, 1), bottom),
                )
                for side in range(2):
                    sums[t, side, head, top_at] = new[side] if first else sums[t, side, head, top_at] + new[side]

    hi_up, hi_down = y_at(1) // 2, y_at(-1) // 2
    low, high = pl.ds(0, 128), pl.ds(128, 128)

    def cuts(t):
        count = 2 if t == LAST else 1
        return [(n, n * 128 // count, 128 // count) for n in range(count)]

    def sum_mine(t):
        for n, at, size in cuts(t):
            here = pl.ds(at, size)
            send(sums.at[t, lo, other, here], q_down.at[t, here], ys.at[t, n], yr.at[t, n], y_peer(1))
            send(
                sums.at[t, lo, other, pl.ds(128 + at, size)], q_up.at[t, here], ys.at[t, 2 + n], yr.at[t, 2 + n], y_peer(-1)
            )

    def sum_theirs(t):
        send(sums.at[t, 1 - lo, hi_up, high], r_down.at[t, high], ys.at[t, 4], yr.at[t, 4], y_peer(1))
        send(sums.at[t, 1 - lo, hi_down, low], r_up.at[t, low], ys.at[t, 5], yr.at[t, 5], y_peer(-1))

    def sum_pass(t):
        for n, at, size in cuts(t):
            here, there = pl.ds(at, size), pl.ds(128 + at, size)
            arrived(q_down.at[t, here], ys.at[t, n], yr.at[t, n], y_peer(-1))
            sums[t, 1 - lo, hi_up, here] = sums[t, 1 - lo, hi_up, here] + q_down[t, here]
            send(sums.at[t, 1 - lo, hi_up, here], r_down.at[t, here], ys.at[t, 6 + n], yr.at[t, 6 + n], y_peer(1))
            arrived(q_up.at[t, here], ys.at[t, 2 + n], yr.at[t, 2 + n], y_peer(1))
            sums[t, 1 - lo, hi_down, there] = sums[t, 1 - lo, hi_down, there] + q_up[t, here]
            send(sums.at[t, 1 - lo, hi_down, there], r_up.at[t, there], ys.at[t, 8 + n], yr.at[t, 8 + n], y_peer(-1))

    def sum_end(t):
        arrived(r_down.at[t, high], ys.at[t, 4], yr.at[t, 4], y_peer(-1))
        arrived(r_up.at[t, low], ys.at[t, 5], yr.at[t, 5], y_peer(1))
        for n, at, size in cuts(t):
            here, there = pl.ds(at, size), pl.ds(128 + at, size)
            arrived(r_down.at[t, here], ys.at[t, 6 + n], yr.at[t, 6 + n], y_peer(-1))
            arrived(r_up.at[t, there], ys.at[t, 8 + n], yr.at[t, 8 + n], y_peer(1))
        total = (sums[t, lo, hi] + r_down[t] + r_up[t]).T.astype(BF16)
        out[64 * t : 64 * (t + 1), 0:half] = total[:64]
        out[64 * t : 64 * (t + 1), half:rows] = total[64:]

    def tiles_whole(tiles):
        for t in tiles:
            z_arrived(t, 3, (0,))
        multiply(tiles, range(8), True)
        for t in tiles:
            sum_mine(t)
            sum_theirs(t)

    def tile_early(t):
        multiply((t,), (0, 1, 2, 6, 7), True)

    def tile_middle(t):
        if t in SPLIT:
            z_arrived(t, 2, range(PARTS // 2, PARTS))
        multiply((t,), (3, 5), False)

    def tile_late(t):
        z_arrived(t, 3, parts_of(t, 3))
        multiply((t,), (4,), False, other)
        sum_mine(t)
        multiply((t,), (4,), False, own)
        sum_theirs(t)

    y_free = 0.0

    def plan_sums(t, begin):
        first = max(y_free, begin)
        plan.at(first + 1.4 + LATENCY_US + PASS_LATE_US, functools.partial(sum_pass, t))
        plan.at(first + 4.2 + LATENCY_US + END_LATE_US if t < 4 else 2e9, functools.partial(sum_end, t))
        return first + 4.2

    for tiles in ((0, 1), (2, 3)):
        when = max(heads_time, max(z_time[t, 3, 0] for t in tiles))
        plan.at(when, functools.partial(tiles_whole, tiles))
        for t in tiles:
            y_free = plan_sums(t, when + 2.5)
    for t in (4, 5, 6):
        last_part = parts_of(t, 2)[-1]
        key = max(z_time[t, 1, last_part], z_key[t, 2, last_part], heads_time + 3.0) + 0.1
        plan.at(key, functools.partial(tile_early, t))
        key = max(key, z_time[t, 2, last_part], z_key[t, 3, parts_of(t, 3)[-1]]) + 0.1
        plan.at(key, functools.partial(tile_middle, t))
        key = max(key, z_time[t, 3, parts_of(t, 3)[-1]]) + 0.1
        plan.at(key, functools.partial(tile_late, t))
        if t != LAST:
            y_free = plan_sums(t, key + 0.6)
    plan.at(1e9, functools.partial(sum_pass, LAST))
    plan.at(3e9, functools.partial(sum_end, LAST))

    plan.run()
    for copy in sent:
        copy.wait_send()


def solution(mesh):
    def per_device(heads, w):
        rows, features = heads.shape
        depth, columns = w.shape
        dma = pltpu.SemaphoreType.DMA
        return pl.pallas_call(
            kernel,
            out_shape=jax.ShapeDtypeStruct((columns // 2, rows), BF16),
            in_specs=[pl.BlockSpec(memory_space=pl.ANY)] * 2,
            out_specs=pl.BlockSpec(memory_space=pltpu.VMEM),
            scratch_shapes=[
                pltpu.VMEM((8, 2, 512, 512), BF16),
                pltpu.VMEM((7, 8, 512, 128), BF16),
                pltpu.VMEM((7, 512, 128), BF16),
                pltpu.VMEM((512, 512), BF16),
                pltpu.VMEM((2, 256, 512), BF16),
                pltpu.VMEM((7, 2, 2, 256, 128), F32),
                pltpu.VMEM((7, 256, 128), F32),
                pltpu.VMEM((7, 256, 128), F32),
                pltpu.VMEM((7, 128, 128), F32),
                pltpu.VMEM((7, 128, 128), F32),
                dma((9,)),
                dma((2, 10, 4)),
                dma((2, 10, 4)),
                dma((2, 2, 3)),
                dma((2, 2, 3)),
                dma((2, 5)),
                dma((2, 5)),
                dma((2, 2)),
                dma((2, 2)),
                dma((7, 10)),
                dma((7, 10)),
            ],
            compiler_params=pltpu.CompilerParams(
                collective_id=0, has_side_effects=True, vmem_limit_bytes=56_000_000
            ),
            name="projection",
        )(heads, w).T

    return jax.shard_map(
        per_device,
        mesh=mesh,
        in_specs=(P("row", ("depth", "col")), P(("depth", "row"), "col")),
        out_specs=P("row", ("col", "depth")),
        check_vma=False,
    )
```
